32 devices in a mesh: span: 32 (over z, y, x, core).
Axes of the slice: x: 2, y: 2, z: 4, core: 2. Of those that a mesh axis runs over, the one named last changes fastest.
Arguments:
- random_slabs: bfloat16 [1024, 4, 3, 2048], P('span'), may hold values from -6 to 6
- span_weights: float32 [513], replicated, may hold values from 0.1 to 2
- wall_filter: bfloat16 [2048, 2048], replicated, may hold values from -0.125 to 0.125
- prev_state: float32 [1024, 3, 2048], P('span'), may hold values from -6 to 6
- time_scale: float32 [3, 2048], replicated, may hold values from 1 to 32
- mean_velocity: float32 [2048], replicated, may hold values from 0 to 2
- lund_diag: float32 [3, 2048], replicated, may hold values from 0.3 to 3
- lund_off: float32 [3, 2048], replicated, may hold values from -1 to 1
Outputs:
- velocity: bfloat16 [1024, 4, 3, 2048], P('span')
- new_state: float32 [1024, 3, 2048], P('span')
The draws below stay inside these ranges and needn't reach their ends.
All inputs are finite; a program needn't handle non-finite values.
Results may differ from the reference program's by a relative error of at most 0.0051.
Values may be sent and summed in bfloat16 or wider, within the bound.
No kernel may reach another device: no remote copies, remote signals or barrier semaphores. Data moves between devices by JAX's collectives and lax.ppermute only.
A program may use at most 128 MiB of HBM per device.

```python
import math
import jax
import jax.numpy as jnp
from jax import lax

NY = 2048
PLANES = 4
NZ = 1024
HALF = 256


def draw_span_weights(key, part):
    offsets = jnp.arange(-HALF, HALF + 1).astype(jnp.float32)
    spread = jnp.float32(HALF)
    envelope = jnp.exp(-jnp.pi * offsets * offsets / (2.0 * spread * spread))
    factor = jnp.exp(jax.random.uniform(key, (2 * HALF + 1,), jnp.float32, math.log(0.5), math.log(2.0)))
    return envelope * factor


def steps_of(rng, shape, cuts, smallest, top_value):
    factor_of, own = 1.0, jax.random.fold_in(rng, 6)
    for position, shards_of in cuts:
        steps = jnp.exp(jax.random.uniform(jax.random.fold_in(own, position), (shards_of,), jnp.float32, smallest / len(cuts), top_value / len(cuts)))
        factor_of = factor_of * jnp.repeat(steps, shape[position] // shards_of).reshape([-1 if axis == position else 1 for axis in range(len(shape))])
    return factor_of


def bell_draw(rng, extent, scale, bound, shards=(), kind=jnp.bfloat16):
    level = steps_of(rng, extent, shards, -0.22, 0.18) if shards else 1.0
    result = jax.random.normal(rng, extent, jnp.float32) * scale * level
    return jnp.minimum(jnp.maximum(result, -bound), bound).astype(kind)


def setup_inputs(seed: int = 0) -> dict:
    key_list = jax.random.split(jax.random.key(seed), 9)
    return {
        "random_slabs": bell_draw(key_list[0], (NZ, PLANES, 3, NY), 1.0, 6.0, ((0, 32),)),
        "span_weights": draw_span_weights(jax.random.fold_in(key_list[8], 71), 0),
        "wall_filter": bell_draw(key_list[2], (NY, NY), NY ** -0.5, 0.125),
        "prev_state": bell_draw(key_list[3], (NZ, 3, NY), 1.0, 6.0, ((0, 32),), jnp.float32),
        "time_scale": jnp.clip(jnp.exp(jax.random.uniform(key_list[4], (3, NY), jnp.float32, math.log(1.0), math.log(32.0))), 1.0, 32.0),
        "mean_velocity": jnp.clip(jax.random.uniform(key_list[5], (NY,), jnp.float32, 0.0, 2.0), 0.0, 2.0),
        "lund_diag": jnp.clip(jnp.exp(jax.random.uniform(key_list[6], (3, NY), jnp.float32, math.log(0.3), math.log(3.0))), 0.3, 3.0),
        "lund_off": jnp.clip(jax.random.uniform(key_list[7], (3, NY), jnp.float32, -1.0, 1.0), -1.0, 1.0),
    }


def normalized_taps(span_weights):
    norm = jnp.sqrt(jnp.sum(span_weights * span_weights))
    return (span_weights / norm).astype(jnp.bfloat16)

def reference(random_slabs, span_weights, wall_filter, prev_state, time_scale, mean_velocity, lund_diag, lund_off):
    total = random_slabs.shape[0]
    taps = lax.optimization_barrier(normalized_taps(span_weights)).astype(jnp.float32)
    middle = jnp.zeros((total - 2 * HALF - 1,), jnp.float32)
    kernel = jnp.concatenate([taps[HALF:], middle, taps[:HALF]])
    kernel_hat = jnp.conj(jnp.fft.rfft(kernel))
    slabs = random_slabs.reshape(total, PLANES * 3, NY).transpose(1, 0, 2)
    wall_wide = wall_filter.astype(jnp.float32)

    def one_slab(slab):
        spectrum = jnp.fft.rfft(slab.astype(jnp.float32), axis=0)
        spanned = jnp.fft.irfft(spectrum * kernel_hat[:, None], n=total, axis=0)
        spanned = lax.optimization_barrier(spanned.astype(jnp.bfloat16)).astype(jnp.float32)
        return jnp.dot(spanned, wall_wide.T, precision=lax.Precision.HIGHEST)
    filtered = lax.map(one_slab, slabs).reshape(PLANES, 3, total, NY)
    decay = jnp.exp(-jnp.pi / (2.0 * time_scale))[:, None, :]
    inject = jnp.sqrt(1.0 - jnp.exp(-jnp.pi / time_scale))[:, None, :]

    def advance(state, plane):
        state = decay * state + inject * plane
        return (state, state)
    final, fluct = lax.scan(advance, prev_state.transpose(1, 0, 2), filtered)
    along = fluct[:, 0]
    normal = fluct[:, 1]
    spanwise = fluct[:, 2]
    first = mean_velocity + lund_diag[0] * along
    second = lund_off[0] * along + lund_diag[1] * normal
    third = lund_off[1] * along + lund_off[2] * normal + lund_diag[2] * spanwise
    velocity = jnp.stack([first, second, third], axis=1).astype(jnp.bfloat16)
    return (velocity.transpose(2, 0, 1, 3), final.transpose(1, 0, 2))
```

```python
import jax
import jax.numpy as jnp
from jax import lax
from jax.experimental import pallas as pl
from jax.experimental.pallas import tpu as pltpu
from jax.sharding import PartitionSpec as P

LANES = 128
VMEM = pl.BlockSpec(memory_space=pltpu.VMEM)
SMEM = pl.BlockSpec(memory_space=pltpu.SMEM)
HBM = pl.BlockSpec(memory_space=pltpu.HBM)


def team_size(count, rows, reach):
    for size in range(1, count + 1):
        if count % size == 0 and rows * size >= reach:
            return size
    return count


def shifted(value, team, by):
    count = lax.axis_size("span")
    return lax.ppermute(value, "span", [(i, (i + by * team) % count) for i in range(count)])


def crossed(value, team, x):
    count = lax.axis_size("span")
    return lax.ppermute(value, "span", [(i, (i // team ^ x) * team + i % team) for i in range(count)])


def within(value, team):
    count = lax.axis_size("span")
    teams = [[first + i for i in range(team)] for first in range(0, count, team)]
    return lax.all_to_all(value, "span", 0, 0, axis_index_groups=teams, tiled=True)


def behind(value, earlier):
    return lax.optimization_barrier((value, earlier))[0]


def kernel_call(body, inputs, outputs, in_specs=None, out_specs=None, scratch=(), flops=1e6, limit=16 << 20):
    moved = sum(a.size * a.dtype.itemsize for a in (*inputs, *outputs))
    return pl.pallas_call(
        body,
        in_specs=in_specs or [VMEM] * len(inputs),
        out_specs=out_specs or [VMEM] * len(outputs),
        out_shape=outputs,
        scratch_shapes=scratch,
        cost_estimate=pl.CostEstimate(flops=int(flops), bytes_accessed=moved, transcendentals=0),
        compiler_params=pltpu.CompilerParams(vmem_limit_bytes=limit),
    )(*inputs)


def band_kernel(taps_ref, band_ref):
    height, length = band_ref.shape
    spread = jnp.broadcast_to(taps_ref[...], (height, length))
    band_ref[...] = pltpu.roll(spread, 0, 1, stride=1, stride_axis=0).astype(jnp.bfloat16)


def band_of(taps, height, reach):
    lead = height - reach
    padded = jnp.pad(taps.astype(jnp.float32), (lead, 3 * height - lead - taps.shape[0]))
    shape = jax.ShapeDtypeStruct((height, 3 * height), jnp.bfloat16)
    return kernel_call(band_kernel, [padded[None]], [shape])[0]


def turned(slabs_ref, turned_ref, put):
    rows, parts, planes, width = slabs_ref.shape
    for part in range(parts):
        for column in range(width // LANES):
            at = slice(column * LANES, (column + 1) * LANES)
            held = turned_ref.at[(part * (width // LANES) + column) % turned_ref.shape[0]]
            for row in range(rows):
                held[pl.ds(row, planes, stride=rows), :] = slabs_ref[row, part, :, at].astype(jnp.float32)
            put(part, column, lambda plane: held[plane * rows : (plane + 1) * rows, :].astype(jnp.bfloat16))


def near_pack_kernel(early, slabs_ref, near_ref, turned_ref):
    parts = slabs_ref.shape[1]
    strip = near_ref.shape[3]

    def put(part, column, value):
        team, inner = divmod(column * LANES, strip)
        for plane in range(early):
            near_ref[team, plane * parts + part, :, inner : inner + LANES] = value(plane)

    turned(slabs_ref, turned_ref, put)


def far_pack_kernel(early, group_ref, slabs_ref, far_ref, turned_ref):
    planes, width = slabs_ref.shape[2:]
    slots = width // far_ref.shape[0] // LANES
    me = group_ref[0]

    def put(part, column, value):
        group, slot = divmod(column, slots)
        for plane in range(early, planes):
            far_ref[me ^ group, (plane - early) * slots + slot, part] = value(plane)

    turned(slabs_ref, turned_ref, put)


def banded(band_ref, blocks):
    height = band_ref.shape[0]
    total = None
    for i, block in enumerate(blocks):
        block = block.reshape(height, block.shape[-1])
        part = jnp.dot(band_ref[:, i * height : (i + 1) * height], block, preferred_element_type=jnp.float32)
        total = part if total is None else total + part
    return total


def near_kernel(band_ref, before_ref, after_ref, own_ref, out_ref):
    for u in range(own_ref.shape[1]):
        total = banded(band_ref, [before_ref[:, u], own_ref[:, u], after_ref[:, u]])
        out_ref[:, u] = total.astype(out_ref.dtype).reshape(out_ref[:, u].shape)


def far_kernel(group_ref, band_ref, held_ref, sent_ref, out_ref, sems):
    groups, units = held_ref.shape[1:3]
    copies = []
    me = group_ref[0]
    height = band_ref.shape[0]
    for q in range(groups):
        blocks = []
        for i in range(3):
            slot = me ^ ((q + i - 1) % groups)
            wide = [held_ref[:, slot, u].reshape(height, LANES) for u in range(units)]
            blocks.append(jnp.concatenate(wide, axis=1))
        total = banded(band_ref, blocks).astype(out_ref.dtype)
        for u in range(units):
            out_ref[:, me ^ q, u] = total[:, u * LANES : (u + 1) * LANES].reshape(out_ref.shape[0], -1, LANES)
        copies.append(pltpu.make_async_copy(out_ref.at[:, me ^ q], sent_ref.at[:, me ^ q], sems.at[q]))
        copies[-1].start()
    for copy in copies:
        copy.wait()


def contract(rows, wall):
    return lax.dot_general(rows, wall, (((1,), (1,)), ((), ())), preferred_element_type=jnp.float32)


def advance(state, fresh, at, scale_ref, mean_ref, diag_ref, off_ref):
    def line(ref, i):
        return ref[i : i + 1, at]

    for i in range(len(state)):
        scale = line(scale_ref, i)
        decay = jnp.exp(-jnp.pi / (2.0 * scale))
        inject = jnp.sqrt(1.0 - jnp.exp(-jnp.pi / scale))
        state[i] = decay * state[i] + inject * fresh[i]
    along, normal, spanwise = state
    first = line(mean_ref, 0) + line(diag_ref, 0) * along
    second = line(off_ref, 0) * along + line(diag_ref, 1) * normal
    third = line(off_ref, 1) * along + line(off_ref, 2) * normal + line(diag_ref, 2) * spanwise
    return state, (first, second, third)


def near_wall_kernel(
    planes, near_ref, wall_ref, state_ref, scale_ref, mean_ref, diag_ref, off_ref, velocity_ref, next_ref, held_ref, sems
):
    team, units, rows, strip = near_ref.shape
    parts = state_ref.shape[0]
    width = wall_ref.shape[0]
    block = 2 * LANES
    copies = []
    for step, start in enumerate(range(0, width, block)):
        at = pl.ds(start, block)
        copies.append(pltpu.make_async_copy(wall_ref.at[at], held_ref.at[at], sems.at[step]))
        copies[-1].start()
    for step, start in enumerate(range(0, width, block)):
        at = slice(start, start + block)
        total = None
        copies[step].wait()
        for i in range(team):
            part = contract(near_ref[i].reshape(units * rows, strip), held_ref[at, i * strip : (i + 1) * strip])
            total = part if total is None else total + part
        state = [state_ref[i, :, at] for i in range(parts)]
        for plane in range(planes):
            fresh = [total[(plane * parts + i) * rows :][:rows] for i in range(parts)]
            state, speeds = advance(state, fresh, at, scale_ref, mean_ref, diag_ref, off_ref)
            for i in range(parts):
                velocity_ref[i, plane * rows : (plane + 1) * rows, at] = speeds[i]
        for i in range(parts):
            next_ref[i, :, at] = state[i]


def far_wall_kernel(
    late, group_ref, *refs
):
    groups = len(refs) - 13
    far_refs = refs[:groups]
    wall_ref, state_ref, early_ref, scale_ref, mean_ref, diag_ref, off_ref = refs[groups : groups + 7]
    velocity_ref, last_ref, turned_ref, speed_ref, final_ref, sems = refs[groups + 7 :]
    parts, rows, width = state_ref.shape
    planes = velocity_ref.shape[2]
    early = planes - late
    slots = far_refs[0].shape[0] // late
    me = group_ref[0]
    block = 2 * LANES
    copies = []
    for step, start in enumerate(range(0, width, block)):
        at = slice(start, start + block)
        total = None
        for k in range(groups):
            for slot in range(0, slots, 2):
                pair = [
                    jnp.concatenate([far_refs[k][p * slots + slot + i].reshape(parts * rows, LANES) for i in range(2)], axis=1)
                    for p in range(late)
                ]
                where = pl.multiple_of((me ^ k) * (slots * LANES) + slot * LANES, 2 * LANES)
                part = contract(jnp.concatenate(pair, axis=0), wall_ref[at, pl.ds(where, 2 * LANES)])
                total = part if total is None else total + part
        state = [state_ref[i, :, at] for i in range(parts)]
        for plane in range(late):
            fresh = [total[(plane * parts + i) * rows :][:rows] for i in range(parts)]
            state, speeds = advance(state, fresh, at, scale_ref, mean_ref, diag_ref, off_ref)
            for i in range(parts):
                for j in range(2):
                    lanes = slice(j * LANES, (j + 1) * LANES)
                    turned_ref[step % 2, i, j, (early + plane) * rows : (early + plane + 1) * rows, :] = speeds[i][:, lanes]
        for i in range(parts):
            final_ref[i, :, at] = state[i]
            for j in range(2):
                lanes = slice(start + j * LANES, start + (j + 1) * LANES)
                turned_ref[step % 2, i, j, : early * rows, :] = early_ref[i, :, lanes]
                for row in range(rows):
                    column = turned_ref[step % 2, i, j, pl.ds(row, planes, stride=rows), :]
                    speed_ref[row, i, :, lanes] = column.astype(speed_ref.dtype)
        here = pltpu.make_async_copy(speed_ref.at[:, :, :, at], velocity_ref.at[:, :, :, at], sems.at[0, step])
        here.start()
        also = pltpu.make_async_copy(final_ref.at[:, :, at], last_ref.at[:, :, at], sems.at[1, step])
        also.start()
        copies += [here, also]
    for copy in copies:
        copy.wait()


def plain(slabs, band, wall_filter, prev_state, time_scale, mean_velocity, lund_diag, lund_off):
    rows, planes, parts, width = slabs.shape
    height = band.shape[0]
    team = height // rows
    strip = width // team
    near = slabs.reshape(rows, planes, parts, team, strip).transpose(3, 1, 2, 0, 4)
    near = within(near.reshape(team, planes * parts, rows, strip), team)
    after = shifted(near, team, -1)
    before = shifted(near, team, 1)
    shape = jax.ShapeDtypeStruct(near.shape, near.dtype)
    near = kernel_call(near_kernel, [band, before, after, near], [shape], limit=32 << 20)[0]
    near = within(near, team).reshape(team, planes, parts, rows, strip)
    near = near.transpose(1, 2, 3, 0, 4).reshape(planes, parts, rows, width)
    filtered = lax.dot_general(near, wall_filter, (((3,), (1,)), ((), ())), preferred_element_type=jnp.float32)
    decay = jnp.exp(-jnp.pi / (2.0 * time_scale))[:, None]
    inject = jnp.sqrt(1.0 - jnp.exp(-jnp.pi / time_scale))[:, None]
    state = prev_state.transpose(1, 0, 2)
    outputs = []
    for plane in range(planes):
        state = decay * state + inject * filtered[plane]
        first = mean_velocity + lund_diag[0] * state[0]
        second = lund_off[0] * state[0] + lund_diag[1] * state[1]
        third = lund_off[1] * state[0] + lund_off[2] * state[1] + lund_diag[2] * state[2]
        outputs.append(jnp.stack([first, second, third]).astype(jnp.bfloat16))
    return (jnp.stack(outputs).transpose(2, 0, 1, 3), state.transpose(1, 0, 2))


def body(
    random_slabs,
    span_weights,
    wall_filter,
    prev_state,
    time_scale,
    mean_velocity,
    lund_diag,
    lund_off,
):
    rows, planes, parts, width = random_slabs.shape
    reach = (span_weights.shape[0] - 1) // 2
    count = lax.axis_size("span")
    team = team_size(count, rows, reach)
    groups = count // team
    height = rows * team
    scaling = jnp.sqrt(jnp.sum(span_weights * span_weights))
    taps = (span_weights / scaling).astype(jnp.bfloat16)
    band = band_of(taps, height, reach)
    group = (lax.axis_index("span") // team).astype(jnp.int32)[None]

    late = planes // 2
    if width != groups * (team // late) * LANES or groups > 4:
        return plain(random_slabs, band, wall_filter, prev_state, time_scale, mean_velocity, lund_diag, lund_off)
    early = planes - late
    strip = width // team
    units = early * parts
    slabs = random_slabs.transpose(0, 2, 1, 3)
    state = prev_state.transpose(1, 0, 2)
    lines = [time_scale, mean_velocity[None], lund_diag, lund_off]
    shape = jax.ShapeDtypeStruct

    turning = [pltpu.VMEM((4, planes * rows, LANES), jnp.float32)]
    far = kernel_call(
        lambda *refs: far_pack_kernel(early, *refs),
        [group, slabs],
        [shape((groups, team, parts, rows, LANES), slabs.dtype)],
        in_specs=[SMEM, VMEM],
        scratch=turning,
    )[0]
    near = kernel_call(
        lambda *refs: near_pack_kernel(early, *refs),
        [slabs],
        [shape((team, units, rows, strip), slabs.dtype)],
        scratch=turning,
    )[0]
    near = within(near, team)
    after = shifted(near, team, -1)
    before = shifted(near, team, 1)
    far = [far[0]] + [crossed(far[x], team, x) for x in range(1, groups)]
    far = within(behind(jnp.stack(far, axis=1), near), team)
    far = kernel_call(
        far_kernel,
        [group, band, far],
        [shape(far.shape, far.dtype)],
        in_specs=[SMEM, VMEM, VMEM],
        out_specs=[HBM],
        scratch=[pltpu.VMEM(far.shape, far.dtype), pltpu.SemaphoreType.DMA((groups,))],
        flops=2 * band.size * far.size // height,
    )[0]
    far = within(far, team)
    near = kernel_call(
        near_kernel,
        [band, before, after, near],
        [shape(near.shape, near.dtype)],
        flops=2 * band.size * near.size // height,
    )[0]
    near = within(behind(near, far), team)
    far = [far[:, 0]] + [crossed(far[:, x], team, x) for x in range(1, groups)]
    speeds, state, wall = kernel_call(
        lambda *refs: near_wall_kernel(early, *refs),
        [near, wall_filter, state, *lines],
        [
            shape((parts, early * rows, width), jnp.float32),
            shape(state.shape, state.dtype),
            shape(wall_filter.shape, wall_filter.dtype),
        ],
        in_specs=[VMEM, HBM] + [VMEM] * 5,
        scratch=[pltpu.SemaphoreType.DMA((width // (2 * LANES),))],
        flops=2 * wall_filter.size * units * rows,
        limit=42 << 20,
    )
    velocity, state = kernel_call(
        lambda *refs: far_wall_kernel(late, *refs),
        [group, *far, wall, state, speeds, *lines],
        [shape(slabs.shape, slabs.dtype), shape(state.shape, state.dtype)],
        in_specs=[SMEM] + [VMEM] * (groups + 7),
        out_specs=[HBM, HBM],
        scratch=[
            pltpu.VMEM((2, parts, 2, planes * rows, LANES), jnp.float32),
            pltpu.VMEM(slabs.shape, slabs.dtype),
            pltpu.VMEM(state.shape, state.dtype),
            pltpu.SemaphoreType.DMA((2, width // (2 * LANES))),
        ],
        flops=2 * wall_filter.size * late * parts * rows,
        limit=24 << 20,
    )
    return (velocity.transpose(0, 2, 1, 3), state.transpose(1, 0, 2))


def solution(mesh):
    placed = (P("span", None, None, None), P(), P(), P("span", None, None), P(), P(), P(), P())
    return jax.shard_map(
        body,
        mesh=mesh,
        in_specs=placed,
        out_specs=(P("span", None, None, None), P("span", None, None)),
        check_vma=False,
    )
```

```python
import jax
import jax.numpy as jnp
from jax import lax
from jax.experimental import pallas as pl
from jax.experimental.pallas import tpu as pltpu
from jax.sharding import PartitionSpec as P

LANES = 128
VMEM = pl.BlockSpec(memory_space=pltpu.VMEM)
SMEM = pl.BlockSpec(memory_space=pltpu.SMEM)
HBM = pl.BlockSpec(memory_space=pltpu.HBM)


def team_size(count, rows, reach):
    for size in range(1, count + 1):
        if count % size == 0 and rows * size >= reach:
            return size
    return count


def shifted(value, team, by):
    count = lax.axis_size("span")
    return lax.ppermute(value, "span", [(i, (i + by * team) % count) for i in range(count)])


def crossed(value, team, x):
    count = lax.axis_size("span")
    return lax.ppermute(value, "span", [(i, (i // team ^ x) * team + i % team) for i in range(count)])


def crossing(pieces, team):
    return [pieces[0]] + [crossed(pieces[x], team, x) for x in range(1, len(pieces))]


def within(value, team):
    count = lax.axis_size("span")
    teams = [[first + i for i in range(team)] for first in range(0, count, team)]
    return lax.all_to_all(value, "span", 0, 0, axis_index_groups=teams, tiled=True)


def direct(pieces):
    count = lax.axis_size("span")
    order = sorted(range(1, len(pieces)), key=lambda x: -x)
    got = list(pieces)
    for x in order:
        got[x] = lax.ppermute(pieces[x], "span", [(i, i ^ x) for i in range(count)])
    return got


def kernel_call(body, inputs, outputs, in_specs=None, out_specs=None, scratch=(), flops=1e6, limit=16 << 20):
    moved = sum(a.size * a.dtype.itemsize for a in (*inputs, *outputs))
    return pl.pallas_call(
        body,
        in_specs=in_specs or [VMEM] * len(inputs),
        out_specs=out_specs or [VMEM] * len(outputs),
        out_shape=outputs,
        scratch_shapes=scratch,
        cost_estimate=pl.CostEstimate(flops=int(flops), bytes_accessed=moved, transcendentals=0),
        compiler_params=pltpu.CompilerParams(vmem_limit_bytes=limit),
    )(*inputs)


def band_kernel(taps_ref, band_ref):
    height, length = band_ref.shape
    spread = jnp.broadcast_to(taps_ref[...], (height, length))
    band_ref[...] = pltpu.roll(spread, 0, 1, stride=1, stride_axis=0).astype(jnp.bfloat16)


def band_of(taps, height, reach):
    lead = height - reach
    padded = jnp.pad(taps.astype(jnp.float32), (lead, 3 * height - lead - taps.shape[0]))
    shape = jax.ShapeDtypeStruct((height, 3 * height), jnp.bfloat16)
    return kernel_call(band_kernel, [padded[None]], [shape])[0]


def turned(slabs_ref, turned_ref, put):
    rows, parts, planes, width = slabs_ref.shape
    for part in range(parts):
        for column in range(width // LANES):
            at = slice(column * LANES, (column + 1) * LANES)
            held = turned_ref.at[(part * (width // LANES) + column) % turned_ref.shape[0]]
            for row in range(rows):
                held[pl.ds(row, planes, stride=rows), :] = slabs_ref[row, part, :, at].astype(jnp.float32)
            put(part, column, lambda plane: held[plane * rows : (plane + 1) * rows, :].astype(jnp.bfloat16))


def near_pack_kernel(early, place_ref, slabs_ref, *refs):
    strips_ref, turned_ref = refs[-2:]
    parts = slabs_ref.shape[1]
    strip = strips_ref.shape[3]

    def put(part, column, value):
        member, inner = divmod(column * LANES, strip)
        for plane in range(early):
            strips_ref[member, plane * parts + part, :, inner : inner + LANES] = value(plane)

    turned(slabs_ref, turned_ref, put)
    for x, ref in enumerate(refs[:-2]):
        ref[...] = strips_ref[place_ref[1] ^ x]


def far_pack_kernel(early, place_ref, slabs_ref, *refs):
    far_ref, turned_ref = refs[-2:]
    planes, width = slabs_ref.shape[2:]
    slots = width // far_ref.shape[0] // LANES

    def put(part, column, value):
        group, slot = divmod(column, slots)
        for plane in range(early, planes):
            member = (plane - early) * slots + slot
            far_ref[group, place_ref[1] ^ member, part] = value(plane)

    turned(slabs_ref, turned_ref, put)
    for k, ref in enumerate(refs[:-2]):
        ref[...] = far_ref[place_ref[0] ^ k]


def join_kernel(*refs):
    for x, ref in enumerate(refs[:-1]):
        refs[-1][x] = ref[...]


def swap_kernel(count, *refs):
    for k, ref in enumerate(refs[:count]):
        for x, out_ref in enumerate(refs[count:]):
            out_ref[k] = ref[x]


def banded(band_ref, blocks):
    height = band_ref.shape[0]
    total = None
    for i, block in enumerate(blocks):
        block = block.reshape(height, block.shape[-1])
        part = jnp.dot(band_ref[:, i * height : (i + 1) * height], block, preferred_element_type=jnp.float32)
        total = part if total is None else total + part
    return total


def near_rows(member, band_ref, before_ref, own_ref, after_ref, out_ref):
    team = own_ref.shape[0]
    for u in range(own_ref.shape[1]):
        blocks = [
            jnp.concatenate([ref[member ^ i, u] for i in range(team)], axis=0) for ref in (before_ref, own_ref, after_ref)
        ]
        out_ref[:, u] = banded(band_ref, blocks).astype(out_ref.dtype).reshape(out_ref[:, u].shape)


def near_kernel(band_ref, before_ref, after_ref, own_ref, out_ref):
    near_rows(0, band_ref, before_ref, own_ref, after_ref, out_ref)


def near_split_kernel(place_ref, band_ref, before_ref, after_ref, own_ref, *refs):
    near_rows(place_ref[1], band_ref, before_ref, own_ref, after_ref, refs[-1])
    for x, ref in enumerate(refs[:-1]):
        ref[...] = refs[-1][place_ref[1] ^ x]


def far_kernel(team, place_ref, band_ref, *refs):
    held_ref, out_ref = refs[2 * team :]
    groups, units = held_ref.shape[1:3]
    me, member = place_ref[0], place_ref[1]
    height = band_ref.shape[0]
    for x in range(team):
        held_ref[member ^ x] = refs[x][...]
    for q in range(groups):
        blocks = []
        for i in range(3):
            slot = me ^ ((q + i - 1) % groups)
            wide = [held_ref[:, slot, u].reshape(height, LANES) for u in range(units)]
            blocks.append(jnp.concatenate(wide, axis=1))
        total = banded(band_ref, blocks).astype(out_ref.dtype)
        for u in range(units):
            out_ref[:, me ^ q, u] = total[:, u * LANES : (u + 1) * LANES].reshape(team, -1, LANES)
    for x in range(team):
        refs[team + x][...] = out_ref[member ^ x]


def contract(rows, wall):
    return lax.dot_general(rows, wall, (((1,), (1,)), ((), ())), preferred_element_type=jnp.float32)


def advance(state, fresh, at, scale_ref, mean_ref, diag_ref, off_ref):
    def line(ref, i):
        return ref[i : i + 1, at]

    for i in range(len(state)):
        scale = line(scale_ref, i)
        decay = jnp.exp(-jnp.pi / (2.0 * scale))
        inject = jnp.sqrt(1.0 - jnp.exp(-jnp.pi / scale))
        state[i] = decay * state[i] + inject * fresh[i]
    along, normal, spanwise = state
    first = line(mean_ref, 0) + line(diag_ref, 0) * along
    second = line(off_ref, 0) * along + line(diag_ref, 1) * normal
    third = line(off_ref, 1) * along + line(off_ref, 2) * normal + line(diag_ref, 2) * spanwise
    return state, (first, second, third)


def stored(speeds, first, step, turned_ref, speed_ref, start):
    rows, parts = speed_ref.shape[:2]
    span = slice(first, first + len(speeds))
    for i in range(parts):
        for j in range(speeds[0][0].shape[1] // LANES):
            held = turned_ref.at[step, i, j]
            for plane, parted in enumerate(speeds):
                held[plane * rows : (plane + 1) * rows, :] = parted[i][:, j * LANES : (j + 1) * LANES]
            lanes = slice(start + j * LANES, start + (j + 1) * LANES)
            for row in range(rows):
                column = held[pl.ds(row, len(speeds), stride=rows), :]
                speed_ref[row, i, span, lanes] = column.astype(speed_ref.dtype)


def far_rows(member, ref, late, slot):
    slots = ref.shape[0] // late
    pair = [
        jnp.concatenate([ref[member ^ (p * slots + slot + i)].reshape(-1, LANES) for i in range(2)], axis=1) for p in range(late)
    ]
    return jnp.concatenate(pair, axis=0)


def far_sum(place_ref, refs, order, late, wall_ref, at, total):
    for k, ref in zip(order, refs):
        slots = ref.shape[0] // late
        for slot in range(0, slots, 2):
            where = pl.multiple_of((place_ref[0] ^ k) * (slots * LANES) + slot * LANES, 2 * LANES)
            part = contract(far_rows(place_ref[1], ref, late, slot), wall_ref[at, pl.ds(where, 2 * LANES)])
            total = part if total is None else total + part
    return total


def far_start_kernel(late, place_ref, own_ref, next_ref, wall_ref, sum_ref, held_ref, sems):
    width = wall_ref.shape[0]
    block = 2 * LANES
    copies = []
    for step, start in enumerate(range(0, width, block)):
        at = pl.ds(start, block)
        copies.append(pltpu.make_async_copy(wall_ref.at[at], held_ref.at[at], sems.at[step]))
        copies[-1].start()
    for step, start in enumerate(range(0, width, block)):
        at = slice(start, start + block)
        copies[step].wait()
        sum_ref[:, at] = far_sum(place_ref, [own_ref, next_ref], [0, 1], late, held_ref, at, None)


def near_wall_kernel(place_ref, *refs):
    near_refs = refs[:-9]
    wall_ref, state_ref, scale_ref, mean_ref, diag_ref, off_ref, speed_ref, next_ref, turned_ref = refs[-9:]
    units, rows, strip = near_refs[0].shape
    parts = state_ref.shape[0]
    width = wall_ref.shape[0]
    block = 2 * LANES
    for step, start in enumerate(range(0, width, block)):
        at = slice(start, start + block)
        total = None
        for x, ref in enumerate(near_refs):
            where = pl.multiple_of((place_ref[1] ^ x) * strip, strip)
            part = contract(ref[...].reshape(units * rows, strip), wall_ref[at, pl.ds(where, strip)])
            total = part if total is None else total + part
        state = [state_ref[i, :, at] for i in range(parts)]
        speeds = []
        for plane in range(units // parts):
            fresh = [total[(plane * parts + i) * rows :][:rows] for i in range(parts)]
            state, parted = advance(state, fresh, at, scale_ref, mean_ref, diag_ref, off_ref)
            speeds.append(parted)
        for i in range(parts):
            next_ref[i, :, at] = state[i]
        stored(speeds, 0, step, turned_ref, speed_ref, start)


def far_wall_kernel(late, count, place_ref, *refs):
    far_refs = refs[:count]
    sum_ref, wall_ref, state_ref, early_ref, scale_ref, mean_ref, diag_ref, off_ref = refs[count : count + 8]
    velocity_ref, last_ref, turned_ref, final_ref, sems = refs[count + 8 :]
    parts, rows, width = state_ref.shape
    early = velocity_ref.shape[2] - late
    block = 2 * LANES
    copies = []
    for step, start in enumerate(range(0, width, block)):
        at = slice(start, start + block)
        order = range(2, 2 + count)
        total = far_sum(place_ref, far_refs, order, late, wall_ref, at, sum_ref[:, at])
        state = [state_ref[i, :, at] for i in range(parts)]
        speeds = []
        for plane in range(late):
            fresh = [total[(plane * parts + i) * rows :][:rows] for i in range(parts)]
            state, parted = advance(state, fresh, at, scale_ref, mean_ref, diag_ref, off_ref)
            speeds.append(parted)
        for i in range(parts):
            final_ref[i, :, at] = state[i]
        stored(speeds, early, step, turned_ref, early_ref, start)
        here = pltpu.make_async_copy(early_ref.at[:, :, :, at], velocity_ref.at[:, :, :, at], sems.at[0, step])
        here.start()
        also = pltpu.make_async_copy(final_ref.at[:, :, at], last_ref.at[:, :, at], sems.at[1, step])
        also.start()
        copies += [here, also]
    for copy in copies:
        copy.wait()


def plain(slabs, band, wall_filter, prev_state, time_scale, mean_velocity, lund_diag, lund_off):
    rows, planes, parts, width = slabs.shape
    height = band.shape[0]
    team = height // rows
    strip = width // team
    near = slabs.reshape(rows, planes, parts, team, strip).transpose(3, 1, 2, 0, 4)
    near = within(near.reshape(team, planes * parts, rows, strip), team)
    after = shifted(near, team, -1)
    before = shifted(near, team, 1)
    shape = jax.ShapeDtypeStruct(near.shape, near.dtype)
    near = kernel_call(near_kernel, [band, before, after, near], [shape], limit=32 << 20)[0]
    near = within(near, team).reshape(team, planes, parts, rows, strip)
    near = near.transpose(1, 2, 3, 0, 4).reshape(planes, parts, rows, width)
    filtered = lax.dot_general(near, wall_filter, (((3,), (1,)), ((), ())), preferred_element_type=jnp.float32)
    decay = jnp.exp(-jnp.pi / (2.0 * time_scale))[:, None]
    inject = jnp.sqrt(1.0 - jnp.exp(-jnp.pi / time_scale))[:, None]
    state = prev_state.transpose(1, 0, 2)
    outputs = []
    for plane in range(planes):
        state = decay * state + inject * filtered[plane]
        first = mean_velocity + lund_diag[0] * state[0]
        second = lund_off[0] * state[0] + lund_diag[1] * state[1]
        third = lund_off[1] * state[0] + lund_off[2] * state[1] + lund_diag[2] * state[2]
        outputs.append(jnp.stack([first, second, third]).astype(jnp.bfloat16))
    return (jnp.stack(outputs).transpose(2, 0, 1, 3), state.transpose(1, 0, 2))


def body(
    random_slabs,
    span_weights,
    wall_filter,
    prev_state,
    time_scale,
    mean_velocity,
    lund_diag,
    lund_off,
):
    rows, planes, parts, width = random_slabs.shape
    reach = (span_weights.shape[0] - 1) // 2
    count = lax.axis_size("span")
    team = team_size(count, rows, reach)
    groups = count // team
    height = rows * team
    scaling = jnp.sqrt(jnp.sum(span_weights * span_weights))
    taps = (span_weights / scaling).astype(jnp.bfloat16)
    band = band_of(taps, height, reach)
    device = lax.axis_index("span")
    place = jnp.stack([device // team, device % team]).astype(jnp.int32)

    late = planes // 2
    if width != groups * (team // late) * LANES or groups > 4:
        return plain(random_slabs, band, wall_filter, prev_state, time_scale, mean_velocity, lund_diag, lund_off)
    early = planes - late
    strip = width // team
    units = early * parts
    slabs = random_slabs.transpose(0, 2, 1, 3)
    state = prev_state.transpose(1, 0, 2)
    lines = [time_scale, mean_velocity[None], lund_diag, lund_off]
    shape = jax.ShapeDtypeStruct

    turning = [pltpu.VMEM((4, planes * rows, LANES), jnp.float32)]
    far = kernel_call(
        lambda *refs: far_pack_kernel(early, *refs),
        [place, slabs],
        [shape((team, parts, rows, LANES), slabs.dtype)] * groups,
        in_specs=[SMEM, VMEM],
        scratch=[pltpu.VMEM((groups, team, parts, rows, LANES), slabs.dtype), *turning],
    )
    near = kernel_call(
        lambda *refs: near_pack_kernel(early, *refs),
        [place, slabs],
        [shape((units, rows, strip), slabs.dtype)] * team,
        in_specs=[SMEM, VMEM],
        scratch=[pltpu.VMEM((team, units, rows, strip), slabs.dtype), *turning],
    )
    far = crossing(far, team)
    near = direct(near)
    near = kernel_call(join_kernel, near, [shape((team, units, rows, strip), slabs.dtype)])[0]
    after = shifted(near, team, -1)
    before = shifted(near, team, 1)
    pieces = [shape((groups, parts, rows, LANES), slabs.dtype)] * team
    far = kernel_call(lambda *refs: swap_kernel(groups, *refs), far, pieces)
    far = direct(far)
    far = kernel_call(
        lambda *refs: far_kernel(team, *refs),
        [place, band, *far],
        pieces,
        in_specs=[SMEM] + [VMEM] * (1 + team),
        scratch=[pltpu.VMEM((team, *pieces[0].shape), slabs.dtype)] * 2,
        flops=2 * band.size * groups * team * parts * rows * LANES // rows,
    )
    far = direct(far)
    far = kernel_call(
        lambda *refs: swap_kernel(team, *refs), far, [shape((team, parts, rows, LANES), slabs.dtype)] * groups
    )
    near = kernel_call(
        near_split_kernel,
        [place, band, before, after, near],
        [shape(near.shape[1:], near.dtype)] * team,
        in_specs=[SMEM] + [VMEM] * 4,
        scratch=[pltpu.VMEM(near.shape, near.dtype)],
        flops=2 * band.size * near.size // height,
    )
    near = direct(near)
    far = crossing(far, team)
    steps = width // (2 * LANES)
    turning = pltpu.VMEM((steps, parts, 2, late * rows, LANES), jnp.float32)
    sums, wall = kernel_call(
        lambda *refs: far_start_kernel(late, *refs),
        [place, far[0], far[1], wall_filter],
        [shape((late * parts * rows, width), jnp.float32), shape(wall_filter.shape, wall_filter.dtype)],
        in_specs=[SMEM, VMEM, VMEM, HBM],
        scratch=[pltpu.SemaphoreType.DMA((steps,))],
        flops=wall_filter.size * late * parts * rows,
        limit=42 << 20,
    )
    speeds, state = kernel_call(
        near_wall_kernel,
        [place, *near, wall, state, *lines],
        [shape(slabs.shape, slabs.dtype), shape(state.shape, state.dtype)],
        in_specs=[SMEM] + [VMEM] * (team + 6),
        scratch=[turning],
        flops=2 * wall_filter.size * units * rows,
    )
    rest = far[2:]
    velocity, state = kernel_call(
        lambda *refs: far_wall_kernel(late, len(rest), *refs),
        [place, *rest, sums, wall, state, speeds, *lines],
        [shape(slabs.shape, slabs.dtype), shape(state.shape, state.dtype)],
        in_specs=[SMEM] + [VMEM] * (len(rest) + 8),
        out_specs=[HBM, HBM],
        scratch=[turning, pltpu.VMEM(state.shape, state.dtype), pltpu.SemaphoreType.DMA((2, steps))],
        flops=wall_filter.size * late * parts * rows,
    )
    return (velocity.transpose(0, 2, 1, 3), state.transpose(1, 0, 2))


def solution(mesh):
    placed = (P("span", None, None, None), P(), P(), P("span", None, None), P(), P(), P(), P())
    return jax.shard_map(
        body,
        mesh=mesh,
        in_specs=placed,
        out_specs=(P("span", None, None, None), P("span", None, None)),
        check_vma=False,
    )
```

```python
import functools

import jax
import jax.numpy as jnp
from jax import lax
from jax.experimental import pallas as pl
from jax.experimental.pallas import tpu as pltpu
from jax.sharding import PartitionSpec as P

LANES = 128
BLOCK = 512
VMEM = pl.BlockSpec(memory_space=pltpu.VMEM)
SMEM = pl.BlockSpec(memory_space=pltpu.SMEM)
HBM = pl.BlockSpec(memory_space=pltpu.HBM)


def team_size(count, rows, reach):
    for size in range(1, count + 1):
        if count % size == 0 and rows * size >= reach:
            return size
    return count


def shifted(value, team, by):
    count = lax.axis_size("span")
    return lax.ppermute(value, "span", [(i, (i + by * team) % count) for i in range(count)])


def crossed(value, team, x):
    count = lax.axis_size("span")
    return lax.ppermute(value, "span", [(i, (i // team ^ x) * team + i % team) for i in range(count)])


def crossing(pieces, team):
    return [pieces[0]] + [crossed(pieces[x], team, x) for x in range(1, len(pieces))]


def within(value, team):
    count = lax.axis_size("span")
    teams = [[first + i for i in range(team)] for first in range(0, count, team)]
    return lax.all_to_all(value, "span", 0, 0, axis_index_groups=teams, tiled=True)


def direct(pieces):
    count = lax.axis_size("span")
    order = sorted(range(1, len(pieces)), key=lambda x: -x)
    got = list(pieces)
    for x in order:
        got[x] = lax.ppermute(pieces[x], "span", [(i, i ^ x) for i in range(count)])
    return got


def placed(body, team):
    def wrapped(index_ref, *refs):
        body((lax.div(index_ref[0], jnp.int32(team)), lax.rem(index_ref[0], jnp.int32(team))), *refs)

    return wrapped


def kernel_call(body, inputs, outputs, in_specs=None, out_specs=None, scratch=(), flops=1e6, limit=16 << 20):
    moved = sum(a.size * a.dtype.itemsize for a in (*inputs, *outputs))
    return pl.pallas_call(
        body,
        in_specs=in_specs or [VMEM] * len(inputs),
        out_specs=out_specs or [VMEM] * len(outputs),
        out_shape=outputs,
        scratch_shapes=scratch,
        cost_estimate=pl.CostEstimate(flops=int(flops), bytes_accessed=moved, transcendentals=0),
        compiler_params=pltpu.CompilerParams(vmem_limit_bytes=limit),
    )(*inputs)


def band_kernel(taps_ref, band_ref):
    height, length = band_ref.shape
    spread = jnp.broadcast_to(taps_ref[...], (height, length))
    band_ref[...] = pltpu.roll(spread, 0, 1, stride=1, stride_axis=0).astype(jnp.bfloat16)


def band_of(taps, height, reach):
    lead = height - reach
    padded = jnp.pad(taps.astype(jnp.float32), (lead, 3 * height - lead - taps.shape[0]))
    shape = jax.ShapeDtypeStruct((height, 3 * height), jnp.bfloat16)
    return kernel_call(band_kernel, [padded[None]], [shape])[0]


def pack_kernel(early, groups, place, slabs_ref, *refs):
    far_ref, near_ref, turned_ref = refs[-3:]
    rows, parts, planes, width = slabs_ref.shape
    strip = near_ref.shape[3]
    slots = width // groups // LANES

    @pl.loop(0, parts)
    def _(part):
        for column in range(width // LANES):
            at = slice(column * LANES, (column + 1) * LANES)
            held = turned_ref.at[column]
            for row in range(rows):
                held[pl.ds(row, planes, stride=rows), :] = slabs_ref[row, part, :, at].astype(jnp.float32)
            member, inner = divmod(column * LANES, strip)
            group, slot = divmod(column, slots)
            for plane in range(planes):
                value = held[plane * rows : (plane + 1) * rows, :].astype(jnp.bfloat16)
                if plane < early:
                    near_ref[member, plane * parts + part, :, inner : inner + LANES] = value
                else:
                    far_ref[group, place[1] ^ ((plane - early) * slots + slot), part] = value

    for k in range(groups):
        refs[k][...] = far_ref[place[0] ^ k]
    for x, ref in enumerate(refs[groups:-3]):
        ref[...] = near_ref[place[1] ^ x]


def fetch_kernel(wall_ref, held_ref, sems):
    rows = wall_ref.shape[0] // sems.shape[0]
    copies = []
    for i in range(sems.shape[0]):
        at = pl.ds(i * rows, rows)
        copies.append(pltpu.make_async_copy(wall_ref.at[at], held_ref.at[at], sems.at[i]))
        copies[-1].start()
    for copy in copies:
        copy.wait()


def join_kernel(*refs):
    for x, ref in enumerate(refs[:-1]):
        refs[-1][x] = ref[...]


def swap_kernel(count, *refs):
    for k, ref in enumerate(refs[:count]):
        for x, out_ref in enumerate(refs[count:]):
            out_ref[k] = ref[x]


def banded(band_ref, blocks):
    height = band_ref.shape[0]
    total = None
    for i, block in enumerate(blocks):
        block = block.reshape(height, block.shape[-1])
        part = jnp.dot(band_ref[:, i * height : (i + 1) * height], block, preferred_element_type=jnp.float32)
        total = part if total is None else total + part
    return total


def near_rows(member, band_ref, before_ref, own_ref, after_ref, out_ref):
    team = own_ref.shape[0]
    for u in range(own_ref.shape[1]):
        blocks = [
            jnp.concatenate([ref[member ^ i, u] for i in range(team)], axis=0) for ref in (before_ref, own_ref, after_ref)
        ]
        out_ref[:, u] = banded(band_ref, blocks).astype(out_ref.dtype).reshape(out_ref[:, u].shape)


def near_kernel(band_ref, before_ref, after_ref, own_ref, out_ref):
    near_rows(0, band_ref, before_ref, own_ref, after_ref, out_ref)


def near_split_kernel(place, band_ref, before_ref, after_ref, own_ref, *refs):
    near_rows(place[1], band_ref, before_ref, own_ref, after_ref, refs[-1])
    for x, ref in enumerate(refs[:-1]):
        ref[...] = refs[-1][place[1] ^ x]


def far_kernel(team, place, band_ref, *refs):
    held_ref, out_ref = refs[2 * team :]
    groups, units = held_ref.shape[1:3]
    me, member = place[0], place[1]
    height = band_ref.shape[0]
    for x in range(team):
        held_ref[member ^ x] = refs[x][...]
    for q in range(groups):
        blocks = []
        for i in range(3):
            slot = me ^ ((q + i - 1) % groups)
            wide = [held_ref[:, slot, u].reshape(height, LANES) for u in range(units)]
            blocks.append(jnp.concatenate(wide, axis=1))
        total = banded(band_ref, blocks).astype(out_ref.dtype)
        for u in range(units):
            out_ref[:, me ^ q, u] = total[:, u * LANES : (u + 1) * LANES].reshape(team, -1, LANES)
    for x in range(team):
        refs[team + x][...] = out_ref[member ^ x]


def contract(rows, wall):
    return lax.dot_general(rows, wall, (((1,), (1,)), ((), ())), preferred_element_type=jnp.float32)


def advance(state, fresh, at, scale_ref, mean_ref, diag_ref, off_ref):
    def line(ref, i):
        return ref[i : i + 1, at]

    for i in range(len(state)):
        scale = line(scale_ref, i)
        decay = jnp.exp(-jnp.pi / (2.0 * scale))
        inject = jnp.sqrt(1.0 - jnp.exp(-jnp.pi / scale))
        state[i] = decay * state[i] + inject * fresh[i]
    along, normal, spanwise = state
    first = line(mean_ref, 0) + line(diag_ref, 0) * along
    second = line(off_ref, 0) * along + line(diag_ref, 1) * normal
    third = line(off_ref, 1) * along + line(off_ref, 2) * normal + line(diag_ref, 2) * spanwise
    return state, (first, second, third)


def far_rows(member, ref, late, slot):
    slots = ref.shape[0] // late
    pair = [
        jnp.concatenate([ref[member ^ (p * slots + slot + i)].reshape(-1, LANES) for i in range(2)], axis=1) for p in range(late)
    ]
    return jnp.concatenate(pair, axis=0)


def far_sum(place, refs, order, late, wall_ref, at, total):
    for k, ref in zip(order, refs):
        slots = ref.shape[0] // late
        for slot in range(0, slots, 2):
            where = pl.multiple_of((place[0] ^ k) * (slots * LANES) + slot * LANES, 2 * LANES)
            part = contract(far_rows(place[1], ref, late, slot), wall_ref[at, pl.ds(where, 2 * LANES)])
            total = part if total is None else total + part
    return total


def far_start_kernel(late, place, own_ref, next_ref, wall_ref, sum_ref):
    width = wall_ref.shape[0]
    block = 2 * LANES
    for start in range(0, width, block):
        at = slice(start, start + block)
        sum_ref[:, at] = far_sum(place, [own_ref, next_ref], [0, 1], late, wall_ref, at, None)


def wall_kernel(late, team, place, *refs):
    near_refs, far_refs = refs[:team], refs[team:-15]
    sum_ref, wall_ref, state_ref, scale_ref, mean_ref, diag_ref, off_ref, velocity_ref, last_ref = refs[-15:-6]
    rows_ref, sums_ref, turned_ref, speed_ref, final_ref, sems = refs[-6:]
    units, rows, strip = near_refs[0].shape
    parts, _, width = state_ref.shape
    planes = velocity_ref.shape[2]
    block = sums_ref.shape[1]
    tiles = block // LANES
    slots = far_refs[0].shape[0] // late
    quarter = slots * LANES
    first = units * rows

    for x, ref in enumerate(near_refs):
        where = pl.multiple_of((place[1] ^ x) * strip, strip)
        rows_ref[:first, pl.ds(where, strip)] = ref[...].reshape(first, strip)
    done = width // quarter - len(far_refs)
    for k, ref in enumerate(far_refs):
        for slot in range(0, slots, 2):
            where = pl.multiple_of((place[0] ^ (done + k)) * quarter + slot * LANES, 2 * LANES)
            rows_ref[first:, pl.ds(where, 2 * LANES)] = far_rows(place[1], ref, late, slot)

    copies = []
    for step, start in enumerate(range(0, width, block)):
        at = slice(start, start + block)
        both = near = None
        for k in range(width // quarter):
            where = pl.ds(pl.multiple_of((place[0] ^ k) * quarter, quarter), quarter)
            if k < done:
                part = contract(rows_ref[:first, where], wall_ref[at, where])
                near = part if near is None else near + part
            else:
                part = contract(rows_ref[:, where], wall_ref[at, where])
                both = part if both is None else both + part
        sums_ref[:first] = both[:first] + near
        sums_ref[first:] = both[first:] + sum_ref[:, at]
        state = [state_ref[i, :, at] for i in range(parts)]
        for plane in range(planes):
            fresh = [sums_ref[(plane * parts + i) * rows :][:rows] for i in range(parts)]
            state, speeds = advance(state, fresh, at, scale_ref, mean_ref, diag_ref, off_ref)
            for i in range(parts):
                for j in range(tiles):
                    value = speeds[i][:, j * LANES : (j + 1) * LANES]
                    turned_ref[i, j, pl.ds(plane, rows, stride=planes), :] = value
        for i in range(parts):
            final_ref[i, :, at] = state[i]
            for j in range(tiles):
                lanes = slice(start + j * LANES, start + (j + 1) * LANES)
                for row in range(rows):
                    column = turned_ref[i, j, row * planes : (row + 1) * planes, :]
                    speed_ref[row, i, :, lanes] = column.astype(speed_ref.dtype)
        here = pltpu.make_async_copy(speed_ref.at[:, :, :, at], velocity_ref.at[:, :, :, at], sems.at[0, step])
        here.start()
        also = pltpu.make_async_copy(final_ref.at[:, :, at], last_ref.at[:, :, at], sems.at[1, step])
        also.start()
        copies += [here, also]
    for copy in copies:
        copy.wait()


def plain(slabs, band, wall_filter, prev_state, time_scale, mean_velocity, lund_diag, lund_off):
    rows, planes, parts, width = slabs.shape
    height = band.shape[0]
    team = height // rows
    strip = width // team
    near = slabs.reshape(rows, planes, parts, team, strip).transpose(3, 1, 2, 0, 4)
    near = within(near.reshape(team, planes * parts, rows, strip), team)
    after = shifted(near, team, -1)
    before = shifted(near, team, 1)
    shape = jax.ShapeDtypeStruct(near.shape, near.dtype)
    near = kernel_call(near_kernel, [band, before, after, near], [shape], limit=32 << 20)[0]
    near = within(near, team).reshape(team, planes, parts, rows, strip)
    near = near.transpose(1, 2, 3, 0, 4).reshape(planes, parts, rows, width)
    filtered = lax.dot_general(near, wall_filter, (((3,), (1,)), ((), ())), preferred_element_type=jnp.float32)
    decay = jnp.exp(-jnp.pi / (2.0 * time_scale))[:, None]
    inject = jnp.sqrt(1.0 - jnp.exp(-jnp.pi / time_scale))[:, None]
    state = prev_state.transpose(1, 0, 2)
    outputs = []
    for plane in range(planes):
        state = decay * state + inject * filtered[plane]
        first = mean_velocity + lund_diag[0] * state[0]
        second = lund_off[0] * state[0] + lund_diag[1] * state[1]
        third = lund_off[1] * state[0] + lund_off[2] * state[1] + lund_diag[2] * state[2]
        outputs.append(jnp.stack([first, second, third]).astype(jnp.bfloat16))
    return (jnp.stack(outputs).transpose(2, 0, 1, 3), state.transpose(1, 0, 2))


def body(
    random_slabs,
    span_weights,
    wall_filter,
    prev_state,
    time_scale,
    mean_velocity,
    lund_diag,
    lund_off,
):
    rows, planes, parts, width = random_slabs.shape
    reach = (span_weights.shape[0] - 1) // 2
    count = lax.axis_size("span")
    team = team_size(count, rows, reach)
    groups = count // team
    height = rows * team
    scaling = jnp.sqrt(jnp.sum(span_weights * span_weights))
    taps = (span_weights / scaling).astype(jnp.bfloat16)
    band = band_of(taps, height, reach)
    place = lax.axis_index("span").astype(jnp.int32)[None]

    late = planes // 2
    if width != groups * (team // late) * LANES or groups > 4:
        return plain(random_slabs, band, wall_filter, prev_state, time_scale, mean_velocity, lund_diag, lund_off)
    early = planes - late
    strip = width // team
    units = early * parts
    slabs = random_slabs.transpose(0, 2, 1, 3)
    state = prev_state.transpose(1, 0, 2)
    lines = [time_scale, mean_velocity[None], lund_diag, lund_off]
    shape = jax.ShapeDtypeStruct

    packed = kernel_call(
        placed(functools.partial(pack_kernel, early, groups), team),
        [place, slabs],
        [shape((team, parts, rows, LANES), slabs.dtype)] * groups + [shape((units, rows, strip), slabs.dtype)] * team,
        in_specs=[SMEM, VMEM],
        scratch=[
            pltpu.VMEM((groups, team, parts, rows, LANES), slabs.dtype),
            pltpu.VMEM((team, units, rows, strip), slabs.dtype),
            pltpu.VMEM((width // LANES, planes * rows, LANES), jnp.float32),
        ],
    )
    far, near = packed[:groups], packed[groups:]
    far = crossing(far, team)
    near = direct(near)
    near = kernel_call(join_kernel, near, [shape((team, units, rows, strip), slabs.dtype)])[0]
    after = shifted(near, team, -1)
    before = shifted(near, team, 1)
    pieces = [shape((groups, parts, rows, LANES), slabs.dtype)] * team
    far = kernel_call(lambda *refs: swap_kernel(groups, *refs), far, pieces)
    far = direct(far)
    wall = kernel_call(
        fetch_kernel,
        [wall_filter],
        [shape(wall_filter.shape, wall_filter.dtype)],
        in_specs=[HBM],
        scratch=[pltpu.SemaphoreType.DMA((4,))],
        limit=42 << 20,
    )[0]
    far = kernel_call(
        placed(functools.partial(far_kernel, team), team),
        [place, band, *far],
        pieces,
        in_specs=[SMEM] + [VMEM] * (1 + team),
        scratch=[pltpu.VMEM((team, *pieces[0].shape), slabs.dtype)] * 2,
        flops=2 * band.size * groups * team * parts * rows * LANES // rows,
    )
    far = direct(far)
    far = kernel_call(
        lambda *refs: swap_kernel(team, *refs), far, [shape((team, parts, rows, LANES), slabs.dtype)] * groups
    )
    near = kernel_call(
        placed(near_split_kernel, team),
        [place, band, before, after, near],
        [shape(near.shape[1:], near.dtype)] * team,
        in_specs=[SMEM] + [VMEM] * 4,
        scratch=[pltpu.VMEM(near.shape, near.dtype)],
        flops=2 * band.size * near.size // height,
    )
    near = direct(near)
    far = crossing(far, team)
    sums = kernel_call(
        placed(functools.partial(far_start_kernel, late), team),
        [place, far[0], far[1], wall],
        [shape((late * parts * rows, width), jnp.float32)],
        in_specs=[SMEM, VMEM, VMEM, VMEM],
        flops=wall_filter.size * late * parts * rows,
    )[0]
    block = BLOCK
    velocity, state = kernel_call(
        placed(functools.partial(wall_kernel, late, team), team),
        [place, *near, *far[2:], sums, wall, state, *lines],
        [shape(slabs.shape, slabs.dtype), shape(state.shape, state.dtype)],
        in_specs=[SMEM] + [VMEM] * (team + groups - 2 + 7),
        out_specs=[HBM, HBM],
        scratch=[
            pltpu.VMEM((planes * parts * rows, width), slabs.dtype),
            pltpu.VMEM((planes * parts * rows, block), jnp.float32),
            pltpu.VMEM((parts, block // LANES, planes * rows, LANES), jnp.float32),
            pltpu.VMEM(slabs.shape, slabs.dtype),
            pltpu.VMEM(state.shape, state.dtype),
            pltpu.SemaphoreType.DMA((2, width // block)),
        ],
        flops=2 * wall_filter.size * planes * parts * rows,
    )
    return (velocity.transpose(0, 2, 1, 3), state.transpose(1, 0, 2))


def solution(mesh):
    placed = (P("span", None, None, None), P(), P(), P("span", None, None), P(), P(), P(), P())
    return jax.shard_map(
        body,
        mesh=mesh,
        in_specs=placed,
        out_specs=(P("span", None, None, None), P("span", None, None)),
        check_vma=False,
    )
```

```python
import functools

import jax
import jax.numpy as jnp
from jax import lax
from jax.experimental import pallas as pl
from jax.experimental.pallas import tpu as pltpu
from jax.sharding import PartitionSpec as P

LANES = 128
BLOCK = 512
VMEM = pl.BlockSpec(memory_space=pltpu.VMEM)
SMEM = pl.BlockSpec(memory_space=pltpu.SMEM)
HBM = pl.BlockSpec(memory_space=pltpu.HBM)


def team_size(count, rows, reach):
    for size in range(1, count + 1):
        if count % size == 0 and rows * size >= reach:
            return size
    return count


def shifted(value, team, by):
    count = lax.axis_size("span")
    return lax.ppermute(value, "span", [(i, (i + by * team) % count) for i in range(count)])


def crossed(value, team, x):
    count = lax.axis_size("span")
    return lax.ppermute(value, "span", [(i, (i // team ^ x) * team + i % team) for i in range(count)])


def crossing(pieces, team):
    got = [pieces[0]]
    for x in range(1, len(pieces)):
        got.append(crossed(pieces[x], team, x))
    return got


def within(value, team):
    count = lax.axis_size("span")
    teams = [[first + i for i in range(team)] for first in range(0, count, team)]
    return lax.all_to_all(value, "span", 0, 0, axis_index_groups=teams, tiled=True)


def direct(pieces):
    count = lax.axis_size("span")
    got = list(pieces)
    for x in range(1, len(pieces)):
        got[x] = lax.ppermute(pieces[x], "span", [(i, i ^ x) for i in range(count)])
    return got


def placed(body, team):
    def wrapped(index_ref, *refs):
        body((lax.div(index_ref[0], jnp.int32(team)), lax.rem(index_ref[0], jnp.int32(team))), *refs)

    return wrapped


def kernel_call(body, inputs, outputs, in_specs=None, out_specs=None, scratch=(), flops=1e6, limit=16 << 20):
    moved = sum(a.size * a.dtype.itemsize for a in (*inputs, *outputs))
    return pl.pallas_call(
        body,
        in_specs=in_specs or [VMEM] * len(inputs),
        out_specs=out_specs or [VMEM] * len(outputs),
        out_shape=outputs,
        scratch_shapes=scratch,
        cost_estimate=pl.CostEstimate(flops=int(flops), bytes_accessed=moved, transcendentals=0),
        compiler_params=pltpu.CompilerParams(vmem_limit_bytes=limit),
    )(*inputs)


def band_kernel(taps_ref, band_ref):
    height, length = band_ref.shape
    spread = jnp.broadcast_to(taps_ref[...], (height, length))
    band_ref[...] = pltpu.roll(spread, 0, 1, stride=1, stride_axis=0).astype(jnp.bfloat16)


def band_of(taps, height, reach):
    lead = height - reach
    padded = jnp.pad(taps.astype(jnp.float32), (lead, 3 * height - lead - taps.shape[0]))
    shape = jax.ShapeDtypeStruct((height, 3 * height), jnp.bfloat16)
    return kernel_call(band_kernel, [padded[None]], [shape])[0]


def pack_kernel(early, groups, place, slabs_ref, *refs):
    slab_ref, far_ref, near_ref, turned_ref, sems = refs[-5:]
    rows, parts, planes, width = slabs_ref.shape
    strip = near_ref.shape[3]
    slots = width // groups // LANES

    def fetch(part):
        return pltpu.make_async_copy(slabs_ref.at[:, part], slab_ref.at[part], sems.at[part])

    for part in range(parts):
        fetch(part).start()

    @pl.loop(0, parts)
    def _(part):
        fetch(part).wait()
        for column in range(width // LANES):
            at = slice(column * LANES, (column + 1) * LANES)
            held = turned_ref.at[column]
            for row in range(rows):
                held[pl.ds(row, planes, stride=rows), :] = slab_ref[part, row, :, at].astype(jnp.float32)
            member, inner = divmod(column * LANES, strip)
            group, slot = divmod(column, slots)
            for plane in range(planes):
                value = held[plane * rows : (plane + 1) * rows, :].astype(jnp.bfloat16)
                if plane < early:
                    near_ref[member, plane * parts + part, :, inner : inner + LANES] = value
                else:
                    far_ref[group, place[1] ^ ((plane - early) * slots + slot), part] = value

    for k in range(groups):
        refs[k][...] = far_ref[place[0] ^ k]
    for x, ref in enumerate(refs[groups:-5]):
        ref[...] = near_ref[place[1] ^ x]


def fetch_kernel(wall_ref, held_ref, sems):
    rows = wall_ref.shape[0] // sems.shape[0]
    copies = []
    for i in range(sems.shape[0]):
        at = pl.ds(i * rows, rows)
        copies.append(pltpu.make_async_copy(wall_ref.at[at], held_ref.at[at], sems.at[i]))
        copies[-1].start()
    for copy in copies:
        copy.wait()


def join_kernel(*refs):
    for x, ref in enumerate(refs[:-1]):
        refs[-1][x] = ref[...]


def swap_kernel(count, *refs):
    for k, ref in enumerate(refs[:count]):
        for x, out_ref in enumerate(refs[count:]):
            out_ref[k] = ref[x]


def banded(band_ref, blocks):
    height = band_ref.shape[0]
    total = None
    for i, block in enumerate(blocks):
        block = block.reshape(height, block.shape[-1])
        part = jnp.dot(band_ref[:, i * height : (i + 1) * height], block, preferred_element_type=jnp.float32)
        total = part if total is None else total + part
    return total


def near_rows(member, band_ref, before_ref, own_ref, after_ref, out_ref):
    team = own_ref.shape[0]
    for u in range(own_ref.shape[1]):
        blocks = [
            jnp.concatenate([ref[member ^ i, u] for i in range(team)], axis=0) for ref in (before_ref, own_ref, after_ref)
        ]
        out_ref[:, u] = banded(band_ref, blocks).astype(out_ref.dtype).reshape(out_ref[:, u].shape)


def near_kernel(band_ref, before_ref, after_ref, own_ref, out_ref):
    near_rows(0, band_ref, before_ref, own_ref, after_ref, out_ref)


def near_split_kernel(place, band_ref, before_ref, after_ref, own_ref, *refs):
    near_rows(place[1], band_ref, before_ref, own_ref, after_ref, refs[-1])
    for x, ref in enumerate(refs[:-1]):
        ref[...] = refs[-1][place[1] ^ x]


def far_kernel(team, place, band_ref, *refs):
    held_ref, out_ref = refs[2 * team :]
    groups, units = held_ref.shape[1:3]
    me, member = place[0], place[1]
    height = band_ref.shape[0]
    for x in range(team):
        held_ref[member ^ x] = refs[x][...]
    for q in range(groups):
        blocks = []
        for i in range(3):
            slot = me ^ ((q + i - 1) % groups)
            wide = [held_ref[:, slot, u].reshape(height, LANES) for u in range(units)]
            blocks.append(jnp.concatenate(wide, axis=1))
        total = banded(band_ref, blocks).astype(out_ref.dtype)
        for u in range(units):
            out_ref[:, me ^ q, u] = total[:, u * LANES : (u + 1) * LANES].reshape(team, -1, LANES)
    for x in range(team):
        refs[team + x][...] = out_ref[member ^ x]


def contract(rows, wall):
    return lax.dot_general(rows, wall, (((1,), (1,)), ((), ())), preferred_element_type=jnp.float32)


def advance(state, fresh, at, scale_ref, mean_ref, diag_ref, off_ref):
    def line(ref, i):
        return ref[i : i + 1, at]

    for i in range(len(state)):
        scale = line(scale_ref, i)
        decay = jnp.exp(-jnp.pi / (2.0 * scale))
        inject = jnp.sqrt(1.0 - jnp.exp(-jnp.pi / scale))
        state[i] = decay * state[i] + inject * fresh[i]
    along, normal, spanwise = state
    first = line(mean_ref, 0) + line(diag_ref, 0) * along
    second = line(off_ref, 0) * along + line(diag_ref, 1) * normal
    third = line(off_ref, 1) * along + line(off_ref, 2) * normal + line(diag_ref, 2) * spanwise
    return state, (first, second, third)


def far_rows(member, ref, late, slot):
    slots = ref.shape[0] // late
    pair = [
        jnp.concatenate([ref[member ^ (p * slots + slot + i)].reshape(-1, LANES) for i in range(2)], axis=1) for p in range(late)
    ]
    return jnp.concatenate(pair, axis=0)


def far_sum(place, refs, order, late, wall_ref, at, total):
    for k, ref in zip(order, refs):
        slots = ref.shape[0] // late
        for slot in range(0, slots, 2):
            where = pl.multiple_of((place[0] ^ k) * (slots * LANES) + slot * LANES, 2 * LANES)
            part = contract(far_rows(place[1], ref, late, slot), wall_ref[at, pl.ds(where, 2 * LANES)])
            total = part if total is None else total + part
    return total


def near_sum(place, refs, order, wall_ref, at):
    total = None
    for x, ref in zip(order, refs):
        units, rows, strip = ref.shape
        where = pl.multiple_of((place[1] ^ x) * strip, strip)
        part = contract(ref[...].reshape(units * rows, strip), wall_ref[at, pl.ds(where, strip)])
        total = part if total is None else total + part
    return total


def wall_start_kernel(late, place, *refs):
    near_refs, far_refs = refs[:-4], refs[-4:-2]
    wall_ref, sum_ref = refs[-2:]
    width = wall_ref.shape[0]
    first = near_refs[0].shape[0] * near_refs[0].shape[1]
    block = 4 * LANES
    for start in range(0, width, block):
        at = slice(start, start + block)
        sum_ref[:first, at] = near_sum(place, near_refs, range(len(near_refs)), wall_ref, at)
        sum_ref[first:, at] = far_sum(place, far_refs, [0, 1], late, wall_ref, at, None)


def wall_kernel(late, team, place, *refs):
    near_refs, far_refs = refs[: team // 2], refs[team // 2 : -14]
    sum_ref, wall_ref, state_ref, scale_ref, mean_ref, diag_ref, off_ref, velocity_ref, last_ref = refs[-14:-5]
    sums_ref, turned_ref, speed_ref, final_ref, sems = refs[-5:]
    units, rows, _ = near_refs[0].shape
    parts, _, width = state_ref.shape
    planes = velocity_ref.shape[2]
    block = sums_ref.shape[1]
    tiles = block // LANES
    first = units * rows

    copies = []
    for step, start in enumerate(range(0, width, block)):
        at = slice(start, start + block)
        order = range(team // 2, team)
        sums_ref[:first] = sum_ref[:first, at] + near_sum(place, near_refs, order, wall_ref, at)
        sums_ref[first:] = far_sum(place, far_refs, [2, 3], late, wall_ref, at, sum_ref[first:, at])
        state = [state_ref[i, :, at] for i in range(parts)]
        for plane in range(planes):
            fresh = [sums_ref[(plane * parts + i) * rows :][:rows] for i in range(parts)]
            state, speeds = advance(state, fresh, at, scale_ref, mean_ref, diag_ref, off_ref)
            for i in range(parts):
                for j in range(tiles):
                    value = speeds[i][:, j * LANES : (j + 1) * LANES]
                    turned_ref[i, j, pl.ds(plane, rows, stride=planes), :] = value
        for i in range(parts):
            final_ref[i, :, at] = state[i]
            for j in range(tiles):
                lanes = slice(start + j * LANES, start + (j + 1) * LANES)
                for row in range(rows):
                    column = turned_ref[i, j, row * planes : (row + 1) * planes, :]
                    speed_ref[row, i, :, lanes] = column.astype(speed_ref.dtype)
        here = pltpu.make_async_copy(speed_ref.at[:, :, :, at], velocity_ref.at[:, :, :, at], sems.at[0, step])
        here.start()
        also = pltpu.make_async_copy(final_ref.at[:, :, at], last_ref.at[:, :, at], sems.at[1, step])
        also.start()
        copies += [here, also]
    for copy in copies:
        copy.wait()


def plain(slabs, band, wall_filter, prev_state, time_scale, mean_velocity, lund_diag, lund_off):
    rows, planes, parts, width = slabs.shape
    height = band.shape[0]
    team = height // rows
    strip = width // team
    near = slabs.reshape(rows, planes, parts, team, strip).transpose(3, 1, 2, 0, 4)
    near = within(near.reshape(team, planes * parts, rows, strip), team)
    after = shifted(near, team, -1)
    before = shifted(near, team, 1)
    shape = jax.ShapeDtypeStruct(near.shape, near.dtype)
    near = kernel_call(near_kernel, [band, before, after, near], [shape], limit=32 << 20)[0]
    near = within(near, team).reshape(team, planes, parts, rows, strip)
    near = near.transpose(1, 2, 3, 0, 4).reshape(planes, parts, rows, width)
    filtered = lax.dot_general(near, wall_filter, (((3,), (1,)), ((), ())), preferred_element_type=jnp.float32)
    decay = jnp.exp(-jnp.pi / (2.0 * time_scale))[:, None]
    inject = jnp.sqrt(1.0 - jnp.exp(-jnp.pi / time_scale))[:, None]
    state = prev_state.transpose(1, 0, 2)
    outputs = []
    for plane in range(planes):
        state = decay * state + inject * filtered[plane]
        first = mean_velocity + lund_diag[0] * state[0]
        second = lund_off[0] * state[0] + lund_diag[1] * state[1]
        third = lund_off[1] * state[0] + lund_off[2] * state[1] + lund_diag[2] * state[2]
        outputs.append(jnp.stack([first, second, third]).astype(jnp.bfloat16))
    return (jnp.stack(outputs).transpose(2, 0, 1, 3), state.transpose(1, 0, 2))


def body(
    random_slabs,
    span_weights,
    wall_filter,
    prev_state,
    time_scale,
    mean_velocity,
    lund_diag,
    lund_off,
):
    rows, planes, parts, width = random_slabs.shape
    reach = (span_weights.shape[0] - 1) // 2
    count = lax.axis_size("span")
    team = team_size(count, rows, reach)
    groups = count // team
    height = rows * team
    scaling = jnp.sqrt(jnp.sum(span_weights * span_weights))
    taps = (span_weights / scaling).astype(jnp.bfloat16)
    band = band_of(taps, height, reach)
    place = lax.axis_index("span").astype(jnp.int32)[None]

    late = planes // 2
    if width != groups * (team // late) * LANES or groups != 4 or team & (team - 1) or width % (2 * team * LANES):
        return plain(random_slabs, band, wall_filter, prev_state, time_scale, mean_velocity, lund_diag, lund_off)
    early = planes - late
    strip = width // team
    units = early * parts
    slabs = random_slabs.transpose(0, 2, 1, 3)
    state = prev_state.transpose(1, 0, 2)
    lines = [time_scale, mean_velocity[None], lund_diag, lund_off]
    shape = jax.ShapeDtypeStruct

    packed = kernel_call(
        placed(functools.partial(pack_kernel, early, groups), team),
        [place, slabs],
        [shape((team, parts, rows, LANES), slabs.dtype)] * groups + [shape((units, rows, strip), slabs.dtype)] * team,
        in_specs=[SMEM, HBM],
        scratch=[
            pltpu.VMEM((parts, rows, planes, width), slabs.dtype),
            pltpu.VMEM((groups, team, parts, rows, LANES), slabs.dtype),
            pltpu.VMEM((team, units, rows, strip), slabs.dtype),
            pltpu.VMEM((width // LANES, planes * rows, LANES), jnp.float32),
            pltpu.SemaphoreType.DMA((parts,)),
        ],
        limit=52 << 20,
    )
    far, near = packed[:groups], packed[groups:]
    far = crossing(far, team)
    near = direct(near)
    near = kernel_call(join_kernel, near, [shape((team, units, rows, strip), slabs.dtype)])[0]
    after = shifted(near, team, -1)
    before = shifted(near, team, 1)
    pieces = [shape((groups, parts, rows, LANES), slabs.dtype)] * team
    far = kernel_call(lambda *refs: swap_kernel(groups, *refs), far, pieces)
    far = direct(far)
    wall = kernel_call(
        fetch_kernel,
        [wall_filter],
        [shape(wall_filter.shape, wall_filter.dtype)],
        in_specs=[HBM],
        scratch=[pltpu.SemaphoreType.DMA((4,))],
        limit=42 << 20,
    )[0]
    far = kernel_call(
        placed(functools.partial(far_kernel, team), team),
        [place, band, *far],
        pieces,
        in_specs=[SMEM] + [VMEM] * (1 + team),
        scratch=[pltpu.VMEM((team, *pieces[0].shape), slabs.dtype)] * 2,
        flops=2 * band.size * groups * team * parts * rows * LANES // rows,
    )
    far = direct(far)
    far = kernel_call(
        lambda *refs: swap_kernel(team, *refs), far, [shape((team, parts, rows, LANES), slabs.dtype)] * groups
    )
    near = kernel_call(
        placed(near_split_kernel, team),
        [place, band, before, after, near],
        [shape(near.shape[1:], near.dtype)] * team,
        in_specs=[SMEM] + [VMEM] * 4,
        scratch=[pltpu.VMEM(near.shape, near.dtype)],
        flops=2 * band.size * near.size // height,
    )
    near = direct(near)
    far = crossing(far, team)
    sums = kernel_call(
        placed(functools.partial(wall_start_kernel, late), team),
        [place, *near[: team // 2], far[0], far[1], wall],
        [shape((planes * parts * rows, width), jnp.float32)],
        in_specs=[SMEM] + [VMEM] * (team // 2 + 3),
        flops=wall_filter.size * planes * parts * rows,
    )[0]
    block = BLOCK
    velocity, state = kernel_call(
        placed(functools.partial(wall_kernel, late, team), team),
        [place, *near[team // 2 :], *far[2:], sums, wall, state, *lines],
        [shape(slabs.shape, slabs.dtype), shape(state.shape, state.dtype)],
        in_specs=[SMEM] + [VMEM] * (team // 2 + groups - 2 + 7),
        out_specs=[HBM, HBM],
        scratch=[
            pltpu.VMEM((planes * parts * rows, block), jnp.float32),
            pltpu.VMEM((parts, block // LANES, planes * rows, LANES), jnp.float32),
            pltpu.VMEM(slabs.shape, slabs.dtype),
            pltpu.VMEM(state.shape, state.dtype),
            pltpu.SemaphoreType.DMA((2, width // block)),
        ],
        flops=2 * wall_filter.size * planes * parts * rows,
    )
    return (velocity.transpose(0, 2, 1, 3), state.transpose(1, 0, 2))


def solution(mesh):
    placed = (P("span", None, None, None), P(), P(), P("span", None, None), P(), P(), P(), P())
    return jax.shard_map(
        body,
        mesh=mesh,
        in_specs=placed,
        out_specs=(P("span", None, None, None), P("span", None, None)),
        check_vma=False,
    )
```

```python
import functools

import jax
import jax.numpy as jnp
from jax import lax
from jax.experimental import pallas as pl
from jax.experimental.pallas import tpu as pltpu
from jax.sharding import PartitionSpec as P

LANES = 128
BLOCK = 512
VMEM = pl.BlockSpec(memory_space=pltpu.VMEM)
SMEM = pl.BlockSpec(memory_space=pltpu.SMEM)
HBM = pl.BlockSpec(memory_space=pltpu.HBM)


def team_size(count, rows, reach):
    for size in range(1, count + 1):
        if count % size == 0 and rows * size >= reach:
            return size
    return count


def shifted(value, team, by):
    count = lax.axis_size("span")
    return lax.ppermute(value, "span", [(i, (i + by * team) % count) for i in range(count)])


def crossed(value, team, x):
    count = lax.axis_size("span")
    return lax.ppermute(value, "span", [(i, (i // team ^ x) * team + i % team) for i in range(count)])


def crossing(pieces, team):
    got = [pieces[0]]
    for x in range(1, len(pieces)):
        got.append(crossed(pieces[x], team, x))
    return got


def within(value, team):
    count = lax.axis_size("span")
    teams = [[first + i for i in range(team)] for first in range(0, count, team)]
    return lax.all_to_all(value, "span", 0, 0, axis_index_groups=teams, tiled=True)


def direct(pieces):
    count = lax.axis_size("span")
    got = list(pieces)
    for x in range(1, len(pieces)):
        got[x] = lax.ppermute(pieces[x], "span", [(i, i ^ x) for i in range(count)])
    return got


def placed(body, team):
    def wrapped(index_ref, *refs):
        body((lax.div(index_ref[0], jnp.int32(team)), lax.rem(index_ref[0], jnp.int32(team))), *refs)

    return wrapped


def kernel_call(body, inputs, outputs, in_specs=None, out_specs=None, scratch=(), flops=1e6, limit=16 << 20):
    moved = sum(a.size * a.dtype.itemsize for a in (*inputs, *outputs))
    return pl.pallas_call(
        body,
        in_specs=in_specs or [VMEM] * len(inputs),
        out_specs=out_specs or [VMEM] * len(outputs),
        out_shape=outputs,
        scratch_shapes=scratch,
        cost_estimate=pl.CostEstimate(flops=int(flops), bytes_accessed=moved, transcendentals=0),
        compiler_params=pltpu.CompilerParams(vmem_limit_bytes=limit),
    )(*inputs)


def band_kernel(taps_ref, band_ref):
    height, length = band_ref.shape
    spread = jnp.broadcast_to(taps_ref[...], (height, length))
    band_ref[...] = pltpu.roll(spread, 0, 1, stride=1, stride_axis=0).astype(jnp.bfloat16)


def band_of(taps, height, reach):
    lead = height - reach
    padded = jnp.pad(taps.astype(jnp.float32), (lead, 3 * height - lead - taps.shape[0]))
    shape = jax.ShapeDtypeStruct((height, 3 * height), jnp.bfloat16)
    return kernel_call(band_kernel, [padded[None]], [shape])[0]


def pack_kernel(early, groups, place, slabs_ref, *refs):
    slab_ref, far_ref, near_ref, turned_ref, sems = refs[-5:]
    rows, parts, planes, width = slabs_ref.shape
    strip = near_ref.shape[3]
    slots = width // groups // LANES

    def fetch(part):
        return pltpu.make_async_copy(slabs_ref.at[:, part], slab_ref.at[part], sems.at[part])

    for part in range(parts):
        fetch(part).start()

    @pl.loop(0, parts)
    def _(part):
        fetch(part).wait()
        for column in range(width // LANES):
            at = slice(column * LANES, (column + 1) * LANES)
            held = turned_ref.at[column]
            for row in range(rows):
                held[pl.ds(row, planes, stride=rows), :] = slab_ref[part, row, :, at].astype(jnp.float32)
            member, inner = divmod(column * LANES, strip)
            group, slot = divmod(column, slots)
            for plane in range(planes):
                value = held[plane * rows : (plane + 1) * rows, :].astype(jnp.bfloat16)
                if plane < early:
                    near_ref[member, plane * parts + part, :, inner : inner + LANES] = value
                else:
                    far_ref[group, place[1] ^ ((plane - early) * slots + slot), part] = value

    for k in range(groups):
        refs[k][...] = far_ref[place[0] ^ k]
    for x, ref in enumerate(refs[groups:-5]):
        ref[...] = near_ref[place[1] ^ x]


def fetch_kernel(wall_ref, held_ref, sems):
    rows = wall_ref.shape[0] // sems.shape[0]
    copies = []
    for i in range(sems.shape[0]):
        at = pl.ds(i * rows, rows)
        copies.append(pltpu.make_async_copy(wall_ref.at[at], held_ref.at[at], sems.at[i]))
        copies[-1].start()
    for copy in copies:
        copy.wait()


def join_kernel(*refs):
    for x, ref in enumerate(refs[:-1]):
        refs[-1][x] = ref[...]


def swap_kernel(count, *refs):
    for k, ref in enumerate(refs[:count]):
        for x, out_ref in enumerate(refs[count:]):
            out_ref[k] = ref[x]


def banded(band_ref, blocks):
    height = band_ref.shape[0]
    total = None
    for i, block in enumerate(blocks):
        block = block.reshape(height, block.shape[-1])
        part = jnp.dot(band_ref[:, i * height : (i + 1) * height], block, preferred_element_type=jnp.float32)
        total = part if total is None else total + part
    return total


def near_rows(member, band_ref, before_ref, own_ref, after_ref, out_ref):
    team = own_ref.shape[0]
    for u in range(own_ref.shape[1]):
        blocks = [
            jnp.concatenate([ref[member ^ i, u] for i in range(team)], axis=0) for ref in (before_ref, own_ref, after_ref)
        ]
        out_ref[:, u] = banded(band_ref, blocks).astype(out_ref.dtype).reshape(out_ref[:, u].shape)


def near_kernel(band_ref, before_ref, after_ref, own_ref, out_ref):
    near_rows(0, band_ref, before_ref, own_ref, after_ref, out_ref)


def near_split_kernel(place, band_ref, before_ref, after_ref, own_ref, *refs):
    near_rows(place[1], band_ref, before_ref, own_ref, after_ref, refs[-1])
    for x, ref in enumerate(refs[:-1]):
        ref[...] = refs[-1][place[1] ^ x]


def far_kernel(team, place, band_ref, *refs):
    held_ref, out_ref = refs[2 * team :]
    groups, units = held_ref.shape[1:3]
    me, member = place[0], place[1]
    height = band_ref.shape[0]
    for x in range(team):
        held_ref[member ^ x] = refs[x][...]
    for q in range(groups):
        blocks = []
        for i in range(3):
            slot = me ^ ((q + i - 1) % groups)
            wide = [held_ref[:, slot, u].reshape(height, LANES) for u in range(units)]
            blocks.append(jnp.concatenate(wide, axis=1))
        total = banded(band_ref, blocks).astype(out_ref.dtype)
        for u in range(units):
            out_ref[:, me ^ q, u] = total[:, u * LANES : (u + 1) * LANES].reshape(team, -1, LANES)
    for x in range(team):
        refs[team + x][...] = out_ref[member ^ x]


def contract(rows, wall):
    return lax.dot_general(rows, wall, (((1,), (1,)), ((), ())), preferred_element_type=jnp.float32)


def rates_of(scale_ref, at):
    rates = []
    for i in range(scale_ref.shape[0]):
        scale = scale_ref[i : i + 1, at]
        rates.append((jnp.exp(-jnp.pi / (2.0 * scale)), jnp.sqrt(1.0 - jnp.exp(-jnp.pi / scale))))
    return rates


def advance(state, fresh, at, rates, mean_ref, diag_ref, off_ref):
    def line(ref, i):
        return ref[i : i + 1, at]

    for i in range(len(state)):
        state[i] = rates[i][0] * state[i] + rates[i][1] * fresh[i]
    along, normal, spanwise = state
    first = line(mean_ref, 0) + line(diag_ref, 0) * along
    second = line(off_ref, 0) * along + line(diag_ref, 1) * normal
    third = line(off_ref, 1) * along + line(off_ref, 2) * normal + line(diag_ref, 2) * spanwise
    return state, (first, second, third)


def far_rows(member, ref, late, slot):
    slots = ref.shape[0] // late
    pair = [
        jnp.concatenate([ref[member ^ (p * slots + slot + i)].reshape(-1, LANES) for i in range(2)], axis=1) for p in range(late)
    ]
    return jnp.concatenate(pair, axis=0)


def far_sum(place, refs, order, late, wall_ref, at, total):
    for k, ref in zip(order, refs):
        slots = ref.shape[0] // late
        for slot in range(0, slots, 2):
            where = pl.multiple_of((place[0] ^ k) * (slots * LANES) + slot * LANES, 2 * LANES)
            part = contract(far_rows(place[1], ref, late, slot), wall_ref[at, pl.ds(where, 2 * LANES)])
            total = part if total is None else total + part
    return total


def near_sum(place, refs, order, wall_ref, at):
    total = None
    for x, ref in zip(order, refs):
        units, rows, strip = ref.shape
        where = pl.multiple_of((place[1] ^ x) * strip, strip)
        part = contract(ref[...].reshape(units * rows, strip), wall_ref[at, pl.ds(where, strip)])
        total = part if total is None else total + part
    return total


def wall_start_kernel(late, place, *refs):
    near_refs, far_refs = refs[:-4], refs[-4:-2]
    wall_ref, sum_ref = refs[-2:]
    width = wall_ref.shape[0]
    first = near_refs[0].shape[0] * near_refs[0].shape[1]
    block = 4 * LANES
    for start in range(0, width, block):
        at = slice(start, start + block)
        sum_ref[:first, at] = near_sum(place, near_refs, range(len(near_refs)), wall_ref, at)
        sum_ref[first:, at] = far_sum(place, far_refs, [0, 1], late, wall_ref, at, None)


def wall_kernel(late, team, place, *refs):
    near_refs, far_refs = refs[: team // 2], refs[team // 2 : -14]
    sum_ref, wall_ref, state_ref, scale_ref, mean_ref, diag_ref, off_ref, velocity_ref, last_ref = refs[-14:-5]
    sums_ref, turned_ref, speed_ref, final_ref, sems = refs[-5:]
    units, rows, _ = near_refs[0].shape
    parts, _, width = state_ref.shape
    planes = velocity_ref.shape[2]
    block = sums_ref.shape[1]
    tiles = block // LANES
    first = units * rows

    copies = []
    for step, start in enumerate(range(0, width, block)):
        at = slice(start, start + block)
        order = range(team // 2, team)
        sums_ref[:first] = sum_ref[:first, at] + near_sum(place, near_refs, order, wall_ref, at)
        sums_ref[first:] = far_sum(place, far_refs, [2, 3], late, wall_ref, at, sum_ref[first:, at])
        state = [state_ref[i, :, at] for i in range(parts)]
        rates = rates_of(scale_ref, at)
        for plane in range(planes):
            fresh = [sums_ref[(plane * parts + i) * rows :][:rows] for i in range(parts)]
            state, speeds = advance(state, fresh, at, rates, mean_ref, diag_ref, off_ref)
            for i in range(parts):
                for j in range(tiles):
                    value = speeds[i][:, j * LANES : (j + 1) * LANES]
                    turned_ref[i, j, pl.ds(plane, rows, stride=planes), :] = value
        for i in range(parts):
            final_ref[i, :, at] = state[i]
            for j in range(tiles):
                lanes = slice(start + j * LANES, start + (j + 1) * LANES)
                for row in range(0, rows, 2):
                    column = turned_ref[i, j, row * planes : (row + 2) * planes, :].astype(speed_ref.dtype)
                    speed_ref[row : row + 2, i, :, lanes] = column.reshape(2, planes, LANES)
        here = pltpu.make_async_copy(speed_ref.at[:, :, :, at], velocity_ref.at[:, :, :, at], sems.at[0, step])
        here.start()
        also = pltpu.make_async_copy(final_ref.at[:, :, at], last_ref.at[:, :, at], sems.at[1, step])
        also.start()
        copies += [here, also]
    for copy in copies:
        copy.wait()


def plain(slabs, band, wall_filter, prev_state, time_scale, mean_velocity, lund_diag, lund_off):
    rows, planes, parts, width = slabs.shape
    height = band.shape[0]
    team = height // rows
    strip = width // team
    near = slabs.reshape(rows, planes, parts, team, strip).transpose(3, 1, 2, 0, 4)
    near = within(near.reshape(team, planes * parts, rows, strip), team)
    after = shifted(near, team, -1)
    before = shifted(near, team, 1)
    shape = jax.ShapeDtypeStruct(near.shape, near.dtype)
    near = kernel_call(near_kernel, [band, before, after, near], [shape], limit=32 << 20)[0]
    near = within(near, team).reshape(team, planes, parts, rows, strip)
    near = near.transpose(1, 2, 3, 0, 4).reshape(planes, parts, rows, width)
    filtered = lax.dot_general(near, wall_filter, (((3,), (1,)), ((), ())), preferred_element_type=jnp.float32)
    decay = jnp.exp(-jnp.pi / (2.0 * time_scale))[:, None]
    inject = jnp.sqrt(1.0 - jnp.exp(-jnp.pi / time_scale))[:, None]
    state = prev_state.transpose(1, 0, 2)
    outputs = []
    for plane in range(planes):
        state = decay * state + inject * filtered[plane]
        first = mean_velocity + lund_diag[0] * state[0]
        second = lund_off[0] * state[0] + lund_diag[1] * state[1]
        third = lund_off[1] * state[0] + lund_off[2] * state[1] + lund_diag[2] * state[2]
        outputs.append(jnp.stack([first, second, third]).astype(jnp.bfloat16))
    return (jnp.stack(outputs).transpose(2, 0, 1, 3), state.transpose(1, 0, 2))


def body(
    random_slabs,
    span_weights,
    wall_filter,
    prev_state,
    time_scale,
    mean_velocity,
    lund_diag,
    lund_off,
):
    rows, planes, parts, width = random_slabs.shape
    reach = (span_weights.shape[0] - 1) // 2
    count = lax.axis_size("span")
    team = team_size(count, rows, reach)
    groups = count // team
    height = rows * team
    scaling = jnp.sqrt(jnp.sum(span_weights * span_weights))
    taps = (span_weights / scaling).astype(jnp.bfloat16)
    band = band_of(taps, height, reach)
    place = lax.axis_index("span").astype(jnp.int32)[None]

    late = planes // 2
    if width != groups * (team // late) * LANES or groups != 4 or team & (team - 1) or width % (2 * team * LANES):
        return plain(random_slabs, band, wall_filter, prev_state, time_scale, mean_velocity, lund_diag, lund_off)
    early = planes - late
    strip = width // team
    units = early * parts
    slabs = random_slabs.transpose(0, 2, 1, 3)
    state = prev_state.transpose(1, 0, 2)
    lines = [time_scale, mean_velocity[None], lund_diag, lund_off]
    shape = jax.ShapeDtypeStruct

    packed = kernel_call(
        placed(functools.partial(pack_kernel, early, groups), team),
        [place, slabs],
        [shape((team, parts, rows, LANES), slabs.dtype)] * groups + [shape((units, rows, strip), slabs.dtype)] * team,
        in_specs=[SMEM, HBM],
        scratch=[
            pltpu.VMEM((parts, rows, planes, width), slabs.dtype),
            pltpu.VMEM((groups, team, parts, rows, LANES), slabs.dtype),
            pltpu.VMEM((team, units, rows, strip), slabs.dtype),
            pltpu.VMEM((width // LANES, planes * rows, LANES), jnp.float32),
            pltpu.SemaphoreType.DMA((parts,)),
        ],
        limit=52 << 20,
    )
    far, near = packed[:groups], packed[groups:]
    far = crossing(far, team)
    near = direct(near)
    near = kernel_call(join_kernel, near, [shape((team, units, rows, strip), slabs.dtype)])[0]
    after = shifted(near, team, -1)
    before = shifted(near, team, 1)
    pieces = [shape((groups, parts, rows, LANES), slabs.dtype)] * team
    far = kernel_call(lambda *refs: swap_kernel(groups, *refs), far, pieces)
    far = direct(far)
    wall = kernel_call(
        fetch_kernel,
        [wall_filter],
        [shape(wall_filter.shape, wall_filter.dtype)],
        in_specs=[HBM],
        scratch=[pltpu.SemaphoreType.DMA((4,))],
        limit=42 << 20,
    )[0]
    far = kernel_call(
        placed(functools.partial(far_kernel, team), team),
        [place, band, *far],
        pieces,
        in_specs=[SMEM] + [VMEM] * (1 + team),
        scratch=[pltpu.VMEM((team, *pieces[0].shape), slabs.dtype)] * 2,
        flops=2 * band.size * groups * team * parts * rows * LANES // rows,
    )
    far = direct(far)
    far = kernel_call(
        lambda *refs: swap_kernel(team, *refs), far, [shape((team, parts, rows, LANES), slabs.dtype)] * groups
    )
    near = kernel_call(
        placed(near_split_kernel, team),
        [place, band, before, after, near],
        [shape(near.shape[1:], near.dtype)] * team,
        in_specs=[SMEM] + [VMEM] * 4,
        scratch=[pltpu.VMEM(near.shape, near.dtype)],
        flops=2 * band.size * near.size // height,
    )
    near = direct(near)
    far = crossing(far, team)
    sums = kernel_call(
        placed(functools.partial(wall_start_kernel, late), team),
        [place, *near[: team // 2], far[0], far[1], wall],
        [shape((planes * parts * rows, width), jnp.float32)],
        in_specs=[SMEM] + [VMEM] * (team // 2 + 3),
        flops=wall_filter.size * planes * parts * rows,
    )[0]
    block = BLOCK
    velocity, state = kernel_call(
        placed(functools.partial(wall_kernel, late, team), team),
        [place, *near[team // 2 :], *far[2:], sums, wall, state, *lines],
        [shape(slabs.shape, slabs.dtype), shape(state.shape, state.dtype)],
        in_specs=[SMEM] + [VMEM] * (team // 2 + groups - 2 + 7),
        out_specs=[HBM, HBM],
        scratch=[
            pltpu.VMEM((planes * parts * rows, block), jnp.float32),
            pltpu.VMEM((parts, block // LANES, planes * rows, LANES), jnp.float32),
            pltpu.VMEM(slabs.shape, slabs.dtype),
            pltpu.VMEM(state.shape, state.dtype),
            pltpu.SemaphoreType.DMA((2, width // block)),
        ],
        flops=2 * wall_filter.size * planes * parts * rows,
    )
    return (velocity.transpose(0, 2, 1, 3), state.transpose(1, 0, 2))


def solution(mesh):
    placed = (P("span", None, None, None), P(), P(), P("span", None, None), P(), P(), P(), P())
    return jax.shard_map(
        body,
        mesh=mesh,
        in_specs=placed,
        out_specs=(P("span", None, None, None), P("span", None, None)),
        check_vma=False,
    )
```
